32 devices in a mesh: rep: 2 (over z, core), dp: 16 (over x, y).
Axes of the slice: x: 4, y: 4, z: 1, core: 2. Of those that a mesh axis runs over, the one named last changes fastest.
The devices are a block of a 4x4x8 slice.
Arguments:
- x: bfloat16 [32, 2048, 1024], P(('rep', 'dp')), parts along dimension 0
- dy: bfloat16 [32, 2048, 1024], P(('rep', 'dp')), parts along dimension 0
- w_gate: bfloat16 [2, 1024, 2816], replicated
- w_up: bfloat16 [2, 1024, 2816], replicated
- w_down: bfloat16 [2, 2816, 1024], replicated
- m_w_gate: float32 [2, 1024, 2816], P(None, 'dp')
- m_w_up: float32 [2, 1024, 2816], P(None, 'dp')
- m_w_down: float32 [2, 2816, 1024], P(None, 'dp')
- v_w_gate: float32 [2, 1024, 2816], P(None, 'dp')
- v_w_up: float32 [2, 1024, 2816], P(None, 'dp')
- v_w_down: float32 [2, 2816, 1024], P(None, 'dp')
Outputs:
- output 1: bfloat16 [4, 1024, 2816], P('rep'), parts along dimension 0
- output 2: bfloat16 [4, 1024, 2816], P('rep'), parts along dimension 0
- output 3: bfloat16 [4, 2816, 1024], P('rep'), parts along dimension 0
- output 4: float32 [4, 1024, 2816], P('rep', 'dp'), parts along dimension 0
- output 5: float32 [4, 1024, 2816], P('rep', 'dp'), parts along dimension 0
- output 6: float32 [4, 2816, 1024], P('rep', 'dp'), parts along dimension 0
- output 7: float32 [4, 1024, 2816], P('rep', 'dp'), parts along dimension 0
- output 8: float32 [4, 1024, 2816], P('rep', 'dp'), parts along dimension 0
- output 9: float32 [4, 2816, 1024], P('rep', 'dp'), parts along dimension 0
There are 2 independent parts. The reference program is written for one: setup_inputs(seed, part) draws one part's arguments, and reference() takes and returns one part's arrays. A program takes and returns all parts, laid end to end along the dimension named above; an argument that names none is the same for every part.
All inputs are finite; a program needn't handle non-finite values.
Results may differ from the reference program's by a relative error of at most 0.02.
Values are sent between devices in bfloat16 or wider.
A program may use at most 768 MiB of HBM per device.

```python
import jax
import jax.numpy as jnp
from jax import lax

SEQUENCES = 16
TOKENS = 2048
D = 1024
FF = 2816
LAYERS = 2
NAMES = ("w_gate", "w_up", "w_down")
SHAPES = {"w_gate": (LAYERS, D, FF), "w_up": (LAYERS, D, FF), "w_down": (LAYERS, FF, D)}


def bump(key, n, height):
    away = (jnp.arange(n, dtype=jnp.int32) - jax.random.randint(key, (), 0, n, jnp.int32)) % n
    return jnp.where(away < n // 8, height, 1.0)


def together(key, own, strength):
    shared = jax.random.normal(key, own.shape[1:], jnp.float32)
    return (own + strength * shared) * lax.rsqrt(1 + strength * strength)


def setup_inputs(seed: int = 0, part: int = 0) -> dict:
    kx, kdy, ka, kb, kz, kf, kh, kl, *keys = jax.random.split(jax.random.key(seed), 8 + 3 * len(NAMES))
    kx, kdy, ka, kb = (jax.random.fold_in(k, part) for k in (kx, kdy, ka, kb))
    kw, km, kv = (keys[i::3] for i in range(3))
    shape = (SEQUENCES, TOKENS, D)
    much_x, much_dy = jax.random.uniform(kz, (2,), jnp.float32, 0.0, 1.0)
    loud = 2.0 ** jax.random.uniform(jax.random.fold_in(kz, 1), (), jnp.float32, -1.0, 2.0)
    layers = 2.0 ** jax.random.uniform(kl, (LAYERS, 1, 1), jnp.float32, -1.0, 1.0)
    x = together(ka, jax.random.normal(kx, shape, jnp.float32), much_x) * bump(kf, D, 4.0)
    dy = together(kb, jax.random.normal(kdy, shape, jnp.float32), much_dy)
    drawn = {"x": x.astype(jnp.bfloat16), "dy": (loud * dy * (SEQUENCES * TOKENS) ** -0.5).astype(jnp.bfloat16)}
    for key, name in zip(kw, NAMES, strict=True):
        w = jax.random.normal(key, SHAPES[name], jnp.float32) * SHAPES[name][1] ** -0.5
        drawn[name] = (w * {"w_gate": 1.0, "w_up": bump(kh, FF, 4.0), "w_down": layers}[name]).astype(jnp.bfloat16)
    for key, name in zip(km, NAMES, strict=True):
        drawn[f"m_{name}"] = 0.1 * jax.random.normal(key, SHAPES[name], jnp.float32)
    for key, name in zip(kv, NAMES, strict=True):
        drawn[f"v_{name}"] = jax.random.uniform(key, SHAPES[name], jnp.float32, 0.005, 0.015)
    return drawn


def matmul(a, w):
    return jnp.dot(a, w, preferred_element_type=jnp.float32).astype(jnp.bfloat16)


def normed(h):
    wide = h.astype(jnp.float32)
    scale = lax.rsqrt(jnp.mean(wide**2, -1, keepdims=True) + 1e-6)
    return (wide * scale).astype(jnp.bfloat16)


def layer(h, w):
    a = normed(h)
    gate = jnp.dot(a, w["w_gate"], preferred_element_type=jnp.float32)
    up = jnp.dot(a, w["w_up"], preferred_element_type=jnp.float32)
    return h + matmul((jax.nn.silu(gate) * up).astype(jnp.bfloat16), w["w_down"])


def adamw(w, m, v, g):
    m = 0.9 * m + 0.1 * g
    v = 0.95 * v + 0.05 * g * g
    step = m * lax.rsqrt(v + 1e-8) + 0.1 * w
    return (w - 0.02 * step).astype(jnp.bfloat16), m, v


def stack(weights, h):
    return lax.scan(lambda h, w: (layer(h, w), None), h, weights)[0]


def reference(x, dy, w_gate, w_up, w_down, m_w_gate, m_w_up, m_w_down, v_w_gate, v_w_up, v_w_down):
    weights = dict(zip(NAMES, (w_gate, w_up, w_down), strict=True))

    def take(so_far, sequence):
        h, by_y = sequence
        _, back = jax.vjp(lambda w: stack(w, h), weights)
        return jax.tree.map(lambda total, term: total + term.astype(jnp.float32), so_far, back(by_y)[0]), None

    none_yet = {name: jnp.zeros(w.shape, jnp.float32) for name, w in weights.items()}
    by_weights, _ = lax.scan(take, none_yet, (x, dy))
    gradients = [by_weights[name].astype(jnp.bfloat16).astype(jnp.float32) for name in NAMES]
    new = [
        adamw(w.astype(jnp.float32), m, v, g)
        for w, m, v, g in zip((w_gate, w_up, w_down), (m_w_gate, m_w_up, m_w_down), (v_w_gate, v_w_up, v_w_down), gradients, strict=True)
    ]
    return tuple(one[which] for which in range(3) for one in new)
```

```python
import functools
import math

import jax
import jax.numpy as jnp
from jax import lax
from jax.experimental import pallas as pl
from jax.experimental.pallas import tpu as pltpu
from jax.sharding import PartitionSpec as P

BF, F32 = jnp.bfloat16, jnp.float32
MESH = pl.DeviceIdType.MESH
TILE = 256


def dot(a, b, dims):
    return lax.dot_general(a, b, (dims, ((), ())), preferred_element_type=F32)


def normed(h):
    wide = h.astype(F32)
    scale = lax.rsqrt(jnp.mean(wide**2, -1, keepdims=True) + 1e-6)
    return (wide * scale).astype(BF), scale


def normed_back(h, scale, da):
    wide, da = h.astype(F32), da.astype(F32)
    inner = jnp.mean(wide * da, -1, keepdims=True)
    return (scale * (da - wide * (scale * scale * inner))).astype(BF)


def gate_up(a, wg, wu):
    return dot(a, wg, ((1,), (0,))), dot(a, wu, ((1,), (0,)))


def back(a, gate, up, hid, dy, wg, wu, wd, deeper):
    d_wd = dot(hid, dy, ((0,), (0,))).astype(BF)
    d_hid = dot(dy, wd, ((1,), (1,))).astype(BF).astype(F32)
    sig = jax.nn.sigmoid(gate)
    d_up = (d_hid * (gate * sig)).astype(BF)
    d_gate = (d_hid * up * (sig * (1 + gate * (1 - sig)))).astype(BF)
    d_wg = dot(a, d_gate, ((0,), (0,))).astype(BF)
    d_wu = dot(a, d_up, ((0,), (0,))).astype(BF)
    da = None
    if deeper:
        da = dot(d_gate, wg, ((1,), (1,))).astype(BF) + dot(d_up, wu, ((1,), (1,))).astype(BF)
    return d_wg, d_wu, d_wd, da


class Flow:
    pass


def sync_kernel(side, tiles, *refs):
    (dwg, dwu, dwd, wg, wu, wd, mg, mu, md, vg, vu, vd,
     og, ou, od, omg, omu, omd, ovg, ovu, ovd,
     L, R1, R2, MV, W, NW, D, R1d, R2d, MVd, Wd, NWd,
     ss, rs, ssd, rsd, ls, lsd, ld, ldd) = refs
    rep, me = lax.axis_index("rep"), lax.axis_index("dp")
    x, y = me // side, me % side

    def mod(v):
        return (v + 2 * side) % side

    def at(xx, yy):
        return (rep, mod(xx) * side + mod(yy))

    barrier = pltpu.get_barrier_semaphore()
    for dx, dy in ((1, 0), (-1, 0), (0, 1), (0, -1)):
        pl.semaphore_signal(barrier, inc=1, device_id=at(x + dx, y + dy), device_id_type=MESH)
    pl.semaphore_wait(barrier, 4)

    slots = tiles

    def tile_of(c, t):
        g = 2 * t + c // 2
        layer = 1 - g // tiles
        return layer, pl.multiple_of((g % tiles) * TILE, TILE)

    gu = Flow()
    gu.local = lambda c, t: L.at[t % 3, c]
    gu.r1 = lambda c, t, s: R1.at[t % 2, c, s]
    gu.r2 = lambda c, t, s: R2.at[t % 2, c, s]
    gu.nw = lambda c, t: NW.at[t % 2, c]
    gu.sems = lambda c, t, k: (ss.at[t % 2, c, k], rs.at[t % 2, c, k])
    gu.mv = lambda c, t: (MV.at[c, 0], MV.at[c, 1])
    gu.w = lambda c, t: W.at[c]
    gu.ls = lambda c, t, k: ls.at[c, k]

    def gu_out(c, t):
        layer, j = tile_of(c, t)
        return (og, ou)[c % 2].at[layer, :, :, :, pl.ds(j, TILE)]

    def gu_hbm(c, t):
        layer, j = tile_of(c, t)
        kind = c % 2
        cut = (layer, slice(None), pl.ds(j, TILE))
        return ((mg, mu)[kind].at[cut], (vg, vu)[kind].at[cut], (wg, wu)[kind].at[layer, x, y, :, pl.ds(j, TILE)],
                (omg, omu)[kind].at[cut], (ovg, ovu)[kind].at[cut])

    gu.out, gu.hbm = gu_out, gu_hbm

    def down(ab):
        fl = Flow()
        lane = lambda c: pl.ds(128 * (4 * ab + c), 128)
        fl.local = lambda c, t: D.at[t, :, :, :, lane(c)]
        fl.r1 = lambda c, t, s: R1d.at[ab, c, s]
        fl.r2 = lambda c, t, s: R2d.at[ab, c, s]
        fl.nw = lambda c, t: NWd.at[ab, c]
        fl.sems = lambda c, t, k: (ssd.at[ab, c, k], rsd.at[ab, c, k])
        fl.mv = lambda c, t: (MVd.at[ab, c, 0], MVd.at[ab, c, 1])
        fl.w = lambda c, t: Wd.at[ab, c]
        fl.ls = lambda c, t, k: lsd.at[ab, c, k]
        fl.out = lambda c, t: od.at[t, :, :, :, lane(c)]

        def hbm(c, t):
            cut = (t, slice(None), lane(c))
            return md.at[cut], vd.at[cut], wd.at[t, x, y, :, lane(c)], omd.at[cut], ovd.at[cut]

        fl.hbm = hbm
        return fl

    downs = (down(0), down(1))

    def stage(fl, c, t, k):
        first, sg = c < 2, (1, -1)[c % 2]
        p1, p2 = (x, y) if first else (y, x)
        along = (at(x + sg, y), at(x, y + sg))
        nb1, nb2 = along if first else along[::-1]
        loc = fl.local(c, t)

        def chunk(ref, q):
            return ref.at[q] if first else ref.at[:, q]

        def sub(ref, q, q2):
            return ref.at[q, q2] if first else ref.at[q2, q]

        def copy(k):
            send, recv = fl.sems(c, t, k)
            if k < 3:
                src, dst, to = chunk(loc, mod(p1 - sg * (1 + k))), fl.r1(c, t, k), nb1
            elif k < 6:
                src, dst, to = sub(loc, p1, mod(p2 - sg * (k - 2))), fl.r2(c, t, k - 3), nb2
            elif k < 9:
                dst, to = sub(fl.out(c, t), p1, mod(p2 - sg * (k - 6))), nb2
                src = fl.nw(c, t) if k == 6 else dst
            else:
                dst, to = chunk(fl.out(c, t), mod(p1 - sg * (k - 9))), nb1
                src = dst
            return pltpu.make_async_remote_copy(src, dst, send, recv, device_id=to, device_id_type=MESH)

        def locals_(ins_too):
            hm, hv, hw, hom, hov = fl.hbm(c, t)
            bm, bv = fl.mv(c, t)
            own = sub(fl.out(c, t), p1, p2)
            s = lambda n: fl.ls(c, t, n)
            if ins_too:
                return [pltpu.make_async_copy(a, b, s(n)) for n, (a, b) in enumerate(((hm, bm), (hv, bv), (hw, fl.w(c, t))))]
            return [pltpu.make_async_copy(a, b, s(3 + n)) for n, (a, b) in enumerate(((bm, hom), (bv, hov), (fl.nw(c, t), own)))]

        if k > 0:
            copy(k - 1).wait()
        if k in (1, 2):
            mine = chunk(loc, mod(p1 - sg * (1 + k)))
            mine[...] = (mine[...].astype(F32) + fl.r1(c, t, k - 1)[...].astype(F32)).astype(BF)
        elif k in (3, 4, 5):
            q2 = mod(p2 - sg * (k - 2))
            mine = sub(loc, p1, q2)
            total = mine[...].astype(F32) + fl.r1(c, t, 2).at[q2][...].astype(F32)
            if k > 3:
                total += fl.r2(c, t, k - 4)[...].astype(F32)
            mine[...] = total.astype(BF)
            if k == 3:
                for one in locals_(True):
                    one.start()
        elif k == 6:
            total = sub(loc, p1, p2)[...].astype(F32) + fl.r1(c, t, 2).at[p2][...].astype(F32)
            g = (total + fl.r2(c, t, 2)[...].astype(F32)).astype(BF).astype(F32)
            for one in locals_(True):
                one.wait()
            bm, bv = fl.mv(c, t)
            m = 0.9 * bm[...] + 0.1 * g
            v = 0.95 * bv[...] + 0.05 * g * g
            w = fl.w(c, t)[...].astype(F32)
            bm[...] = m
            bv[...] = v
            fl.nw(c, t)[...] = (w - 0.02 * (m * lax.rsqrt(v + 1e-8) + 0.1 * w)).astype(BF)
            for one in locals_(False):
                one.start()
        elif k == 7:
            for one in locals_(False):
                one.wait()
        if k < 12:
            copy(k).start()

    def load(c, t):
        layer, j = tile_of(c, t)
        return pltpu.make_async_copy((dwg, dwu)[c % 2].at[layer, :, :, :, pl.ds(j, TILE)], L.at[t % 3, c], ld.at[t % 2, c])

    for layer in (0, 1):
        pltpu.make_async_copy(dwd.at[layer], D.at[layer], ldd.at[layer]).start()

    def round_(i, rho):
        for k in range(12, -1, -1):
            for pair in (0, 1):
                off = 2 + 2 * pair
                if (k + off) % 4 == rho:
                    t = i - (k + off) // 4

                    @pl.when((t >= 0) & (t < slots))
                    def _():
                        for c in (2 * pair, 2 * pair + 1):
                            if k == 0:
                                load(c, t).wait()
                            stage(gu, c, t, k)
            for ab in (0, 1):
                off = 2 * ab
                if (k + off) % 4 == rho:
                    i0 = i - (k + off) // 4
                    a, b = (tiles + 1) // 2, tiles

                    @pl.when((i0 == a) | (i0 == b))
                    def _():
                        layer = jnp.where(i0 == a, 1, 0)
                        if k == 0 and ab == 0:
                            pltpu.make_async_copy(dwd.at[layer], D.at[layer], ldd.at[layer]).wait()
                        for c in range(4):
                            stage(downs[ab], c, layer, k)

    def turn(i, carry):
        @pl.when(i < slots)
        def _():
            for c in range(4):
                load(c, i).start()

        for rho in range(4):
            round_(i, rho)
        return carry

    lax.fori_loop(0, slots + 4, turn, 0)


def synced(mesh, d_ws, ws, ms, vs):
    n = mesh.shape["dp"]
    side = math.isqrt(n)
    layers, d, ff = ws[0].shape
    tiles = ff // TILE
    cut = lambda a: a.reshape(layers, side, side, a.shape[1] // n, a.shape[2])
    rows, rowsd = d // n, ff // n
    hbm = pl.BlockSpec(memory_space=pl.ANY)
    ws5 = [cut(w) for w in ws]
    out_shape = [jax.ShapeDtypeStruct(w.shape, BF) for w in ws5] + [jax.ShapeDtypeStruct(m.shape, F32) for m in (*ms, *vs)]
    gu, dn = (rows, TILE), (rowsd, 128)
    dma = pltpu.SemaphoreType.DMA
    scratch = [
        pltpu.VMEM((3, 4, side, side, *gu), BF),
        pltpu.VMEM((2, 4, 3, side, *gu), BF),
        pltpu.VMEM((2, 4, 3, *gu), BF),
        pltpu.VMEM((4, 2, *gu), F32),
        pltpu.VMEM((4, *gu), BF),
        pltpu.VMEM((2, 4, *gu), BF),
        pltpu.VMEM((layers, side, side, rowsd, d), BF),
        pltpu.VMEM((2, 4, 3, side, *dn), BF),
        pltpu.VMEM((2, 4, 3, *dn), BF),
        pltpu.VMEM((2, 4, 2, *dn), F32),
        pltpu.VMEM((2, 4, *dn), BF),
        pltpu.VMEM((2, 4, *dn), BF),
        dma((2, 4, 12)), dma((2, 4, 12)), dma((2, 4, 12)), dma((2, 4, 12)),
        dma((4, 6)), dma((2, 4, 6)), dma((2, 4)), dma((2,)),
    ]
    res = pl.pallas_call(
        functools.partial(sync_kernel, side, tiles),
        out_shape=out_shape,
        in_specs=[hbm] * 12,
        out_specs=[hbm] * 9,
        scratch_shapes=scratch,
        compiler_params=pltpu.CompilerParams(collective_id=0, has_side_effects=True, vmem_limit_bytes=60 * 2**20),
        name="sync",
    )(*(cut(g) for g in d_ws), *ws5, *ms, *vs)
    return [r.reshape(w.shape) for r, w in zip(res[:3], ws)] + list(res[3:])


def solution(mesh):
    def step(x, dy, wg, wu, wd, *mv):
        x, dy = x[0], dy[0]
        a0, s0 = normed(x)
        g0, u0 = gate_up(a0, wg[0], wu[0])
        hid0 = (jax.nn.silu(g0) * u0).astype(BF)
        h1 = x + dot(hid0, wd[0], ((1,), (0,))).astype(BF)
        a1, s1 = normed(h1)
        g1, u1 = gate_up(a1, wg[1], wu[1])
        hid1 = (jax.nn.silu(g1) * u1).astype(BF)
        d_wg1, d_wu1, d_wd1, da = back(a1, g1, u1, hid1, dy, wg[1], wu[1], wd[1], True)
        dh1 = dy + normed_back(h1, s1, da)
        d_wg0, d_wu0, d_wd0, _ = back(a0, g0, u0, hid0, dh1, wg[0], wu[0], wd[0], False)
        grads = [jnp.stack(p) for p in ((d_wg0, d_wg1), (d_wu0, d_wu1), (d_wd0, d_wd1))]
        return tuple(synced(mesh, grads, (wg, wu, wd), mv[:3], mv[3:]))

    rd, rep, shard = P(("rep", "dp")), P(), P(None, "dp", None)
    out, outs = P("rep"), P("rep", "dp", None)
    return jax.shard_map(
        step,
        mesh=mesh,
        in_specs=(rd, rd, rep, rep, rep, *[shard] * 6),
        out_specs=(out, out, out, *[outs] * 6),
        check_vma=False,
    )
```

```python
import functools
import math

import jax
import jax.numpy as jnp
from jax import lax
from jax.experimental import pallas as pl
from jax.experimental.pallas import tpu as pltpu
from jax.sharding import PartitionSpec as P

BF, F32 = jnp.bfloat16, jnp.float32
MESH = pl.DeviceIdType.MESH
TILE = 256


def dot(a, b, dims):
    return lax.dot_general(a, b, (dims, ((), ())), preferred_element_type=F32)


def normed(h):
    wide = h.astype(F32)
    scale = lax.rsqrt(jnp.mean(wide**2, -1, keepdims=True) + 1e-6)
    return (wide * scale).astype(BF), scale


def gate_up(a, wg, wu):
    return dot(a, wg, ((1,), (0,))), dot(a, wu, ((1,), (0,)))


class Flow:
    pass


def sync_kernel(side, tiles, *refs):
    (a1, a1t, a0, a0t, dy_in, h1, wg2, wu2, wd2, wg, wu, wd, mg, mu, md, vg, vu, vd,
     og, ou, od, omg, omu, omd, ovg, ovu, ovd,
     L, R1, R2, MV, W, NW, D, R1d, R2d, MVd, Wd, NWd, A, AT, DY, DA, HT, DGU, TW, TD,
     ss, rs, ssd, rsd, ls, lsd, lt, la) = refs
    tokens, d = A.shape
    block = 512
    rep, me = lax.axis_index("rep"), lax.axis_index("dp")
    x, y = me // side, me % side

    def mod(v):
        return (v + 2 * side) % side

    def at(xx, yy):
        return (rep, mod(xx) * side + mod(yy))

    for src, dst, sem in ((a1, A, la.at[0]), (a1t, AT, la.at[1]), (dy_in, DY, la.at[2])):
        pltpu.make_async_copy(src, dst, sem).start()
    barrier = pltpu.get_barrier_semaphore()
    for dx, dy in ((1, 0), (-1, 0), (0, 1), (0, -1)):
        pl.semaphore_signal(barrier, inc=1, device_id=at(x + dx, y + dy), device_id_type=MESH)
    DA[...] = jnp.zeros_like(DA)
    pl.semaphore_wait(barrier, 4)

    slots = tiles

    def tile_of(c, t):
        g = 2 * t + c // 2
        layer = 1 - g // tiles
        return layer, pl.multiple_of((g % tiles) * TILE, TILE)

    gu = Flow()
    gu.local = lambda c, t: L.at[t % 3, c]
    gu.r1 = lambda c, t, s: R1.at[t % 2, c, s]
    gu.r2 = lambda c, t, s: R2.at[t % 2, c, s]
    gu.nw = lambda c, t: NW.at[t % 2, c]
    gu.sems = lambda c, t, k: (ss.at[t % 2, c, k], rs.at[t % 2, c, k])
    gu.mv = lambda c, t: (MV.at[c, 0], MV.at[c, 1])
    gu.w = lambda c, t: W.at[c]
    gu.ls = lambda c, t, k: ls.at[c, k]

    def gu_out(c, t):
        layer, j = tile_of(c, t)
        return (og, ou)[c % 2].at[layer, :, :, :, pl.ds(j, TILE)]

    def gu_hbm(c, t):
        layer, j = tile_of(c, t)
        kind = c % 2
        cut = (layer, slice(None), pl.ds(j, TILE))
        return ((mg, mu)[kind].at[cut], (vg, vu)[kind].at[cut], (wg, wu)[kind].at[layer, x, y, :, pl.ds(j, TILE)],
                (omg, omu)[kind].at[cut], (ovg, ovu)[kind].at[cut])

    gu.out, gu.hbm = gu_out, gu_hbm

    def down(ab):
        fl = Flow()
        lane = lambda c: pl.ds(128 * (4 * ab + c), 128)
        fl.local = lambda c, t: D.at[t, :, :, :, :, lane(c)]
        fl.r1 = lambda c, t, s: R1d.at[ab, c, s]
        fl.r2 = lambda c, t, s: R2d.at[ab, c, s]
        fl.nw = lambda c, t: NWd.at[ab, c]
        fl.sems = lambda c, t, k: (ssd.at[ab, c, k], rsd.at[ab, c, k])
        fl.mv = lambda c, t: (MVd.at[ab, c, 0], MVd.at[ab, c, 1])
        fl.w = lambda c, t: Wd.at[ab, c]
        fl.ls = lambda c, t, k: lsd.at[ab, c, k]
        fl.out = lambda c, t: od.at[t, :, :, :, :, lane(c)]

        def hbm(c, t):
            cut = (t, slice(None), slice(None), lane(c))
            return md.at[cut], vd.at[cut], wd.at[t, x, y, :, :, lane(c)], omd.at[cut], ovd.at[cut]

        fl.hbm = hbm
        return fl

    downs = (down(0), down(1))

    def stage(fl, c, t, k):
        first, sg = c < 2, (1, -1)[c % 2]
        p1, p2 = (x, y) if first else (y, x)
        along = (at(x + sg, y), at(x, y + sg))
        nb1, nb2 = along if first else along[::-1]
        loc = fl.local(c, t)

        def chunk(ref, q):
            return ref.at[q] if first else ref.at[:, q]

        def sub(ref, q, q2):
            return ref.at[q, q2] if first else ref.at[q2, q]

        def copy(k):
            send, recv = fl.sems(c, t, k)
            if k < 3:
                src, dst, to = chunk(loc, mod(p1 - sg * (1 + k))), fl.r1(c, t, k), nb1
            elif k < 6:
                src, dst, to = sub(loc, p1, mod(p2 - sg * (k - 2))), fl.r2(c, t, k - 3), nb2
            elif k < 9:
                dst, to = sub(fl.out(c, t), p1, mod(p2 - sg * (k - 6))), nb2
                src = fl.nw(c, t) if k == 6 else dst
            else:
                dst, to = chunk(fl.out(c, t), mod(p1 - sg * (k - 9))), nb1
                src = dst
            return pltpu.make_async_remote_copy(src, dst, send, recv, device_id=to, device_id_type=MESH)

        def locals_(ins_too):
            hm, hv, hw, hom, hov = fl.hbm(c, t)
            bm, bv = fl.mv(c, t)
            own = sub(fl.out(c, t), p1, p2)
            s = lambda n: fl.ls(c, t, n)
            if ins_too:
                return [pltpu.make_async_copy(a, b, s(n)) for n, (a, b) in enumerate(((hm, bm), (hv, bv), (hw, fl.w(c, t))))]
            return [pltpu.make_async_copy(a, b, s(3 + n)) for n, (a, b) in enumerate(((bm, hom), (bv, hov), (fl.nw(c, t), own)))]

        if k > 0:
            copy(k - 1).wait()
        if k in (1, 2):
            mine = chunk(loc, mod(p1 - sg * (1 + k)))
            mine[...] = (mine[...].astype(F32) + fl.r1(c, t, k - 1)[...].astype(F32)).astype(BF)
        elif k in (3, 4, 5):
            q2 = mod(p2 - sg * (k - 2))
            mine = sub(loc, p1, q2)
            total = mine[...].astype(F32) + fl.r1(c, t, 2).at[q2][...].astype(F32)
            if k > 3:
                total += fl.r2(c, t, k - 4)[...].astype(F32)
            mine[...] = total.astype(BF)
            if k == 3:
                for one in locals_(True):
                    one.start()
        elif k == 6:
            total = sub(loc, p1, p2)[...].astype(F32) + fl.r1(c, t, 2).at[p2][...].astype(F32)
            g = (total + fl.r2(c, t, 2)[...].astype(F32)).astype(BF).astype(F32)
            for one in locals_(True):
                one.wait()
            bm, bv = fl.mv(c, t)
            m = 0.9 * bm[...] + 0.1 * g
            v = 0.95 * bv[...] + 0.05 * g * g
            w = fl.w(c, t)[...].astype(F32)
            bm[...] = m
            bv[...] = v
            fl.nw(c, t)[...] = (w - 0.02 * (m * lax.rsqrt(v + 1e-8) + 0.1 * w)).astype(BF)
            for one in locals_(False):
                one.start()
        elif k == 7:
            for one in locals_(False):
                one.wait()
        if k < 12:
            copy(k).start()

    def tile_loads(g):
        layer, j, par = 1 - g // tiles, pl.multiple_of((g % tiles) * TILE, TILE), g % 2
        cols = pl.ds(j, TILE)
        return (pltpu.make_async_copy(wg2.at[layer, :, cols], TW.at[par, :, :TILE], lt.at[par, 0]),
                pltpu.make_async_copy(wu2.at[layer, :, cols], TW.at[par, :, TILE:], lt.at[par, 1]),
                pltpu.make_async_copy(wd2.at[layer, cols, :], TD.at[par], lt.at[par, 2]))

    def state_load(n):
        src, dst = ((a1, A), (a1t, AT), (dy_in, DY), (h1, A), (a0, A), (a0t, AT))[n]
        return pltpu.make_async_copy(src, dst, la.at[n])

    def forth_and_back(g):
        layer, par = 1 - g // tiles, g % 2

        @pl.when(g + 1 < 2 * tiles)
        def _():
            for one in tile_loads(g + 1):
                one.start()

        for one in tile_loads(g):
            one.wait()

        def some(b, carry):
            rows = pl.ds(pl.multiple_of(b * block, block), block)
            both = dot(A[rows, :], TW[par], ((1,), (0,)))
            gate, up = both[:, :TILE], both[:, TILE:]
            d_hid = dot(DY[rows, :], TD[par], ((1,), (1,))).astype(BF).astype(F32)
            sig = jax.nn.sigmoid(gate)
            silu = gate * sig
            HT[:, rows] = (silu * up).astype(BF).T
            DGU[rows, TILE:] = (d_hid * silu).astype(BF)
            DGU[rows, :TILE] = (d_hid * up * (sig * (1 + gate * (1 - sig)))).astype(BF)

            @pl.when(layer == 1)
            def _():
                DA[rows, :] += dot(DGU[rows, :], TW[par], ((1,), (1,)))

            return carry

        lax.fori_loop(0, tokens // block, some, 0)

    def gradients(g, slot, c):
        layer, j = 1 - g // tiles, g % tiles
        rows = TILE // 16

        def of_gate_and_up(q, carry):
            both = dot(AT[pl.ds(pl.multiple_of(q * 256, 256), 256), :], DGU[...], ((1,), (0,))).astype(BF)
            L[slot % 3, c, q] = both[:, :TILE].reshape(side, -1, TILE)
            L[slot % 3, c + 1, q] = both[:, TILE:].reshape(side, -1, TILE)
            return carry

        lax.fori_loop(0, side, of_gate_and_up, 0)

        def of_down(n, carry):
            lanes = pl.ds(pl.multiple_of(n * 256, 256), 256)
            one = dot(HT[...], DY[:, lanes], ((1,), (0,))).astype(BF)
            for i in range(rows):
                r = j * rows + i
                per = D.shape[3]
                D[layer, r // (side * per), (r // per) % side, r % per, :, lanes] = one[16 * i : 16 * i + 16]
            return carry

        lax.fori_loop(0, d // 256, of_down, 0)

    def to_the_first_layer():
        state_load(3).start()
        state_load(3).wait()

        def some(b, carry):
            rows = pl.ds(pl.multiple_of(b * 256, 256), 256)
            h = A[rows, :].astype(F32)
            scale = lax.rsqrt(jnp.mean(h * h, -1, keepdims=True) + 1e-6)
            da = DA[rows, :].astype(BF).astype(F32)
            inner = jnp.mean(h * da, -1, keepdims=True)
            back = (scale * (da - h * (scale * scale * inner))).astype(BF)
            DY[rows, :] = (DY[rows, :].astype(F32) + back.astype(F32)).astype(BF)
            return carry

        lax.fori_loop(0, tokens // 256, some, 0)
        for n in (4, 5):
            state_load(n).start()
        for n in (4, 5):
            state_load(n).wait()

    def round_(i, rho):
        for k in range(12, -1, -1):
            for pair in (0, 1):
                off = 2 + 2 * pair
                if (k + off) % 4 == rho:
                    t = i - (k + off) // 4

                    @pl.when((t >= 0) & (t < slots))
                    def _():
                        for c in (2 * pair, 2 * pair + 1):
                            stage(gu, c, t, k)
            for ab in (0, 1):
                off = 2 * ab
                if (k + off) % 4 == rho:
                    i0 = i - (k + off) // 4
                    a, b = (tiles + 1) // 2, tiles

                    @pl.when((i0 == a) | (i0 == b))
                    def _():
                        layer = jnp.where(i0 == a, 1, 0)
                        for c in range(4):
                            stage(downs[ab], c, layer, k)

    def turn(i, carry):
        for half in (0, 1):
            g = 2 * i + half
            round_(i, 2 * half)

            if half:
                @pl.when(g == tiles)
                def _():
                    to_the_first_layer()

            @pl.when(i < slots)
            def _():
                forth_and_back(g)

            round_(i, 2 * half + 1)

            @pl.when(i < slots)
            def _():
                gradients(g, i, 2 * half)

        return carry

    for one in tile_loads(0):
        one.start()
    for n in range(3):
        state_load(n).wait()
    lax.fori_loop(0, slots + 4, turn, 0)


def synced(mesh, states, ws, ms, vs):
    n = mesh.shape["dp"]
    side = math.isqrt(n)
    layers, d, ff = ws[0].shape
    tokens = states[0].shape[0]
    tiles = ff // TILE
    rows, per = d // n, ff // n // 16
    gu, dn = (rows, TILE), (per, 16, 128)
    mats = ((rows, ff), (rows, ff), (per, 16, d))
    hbm = pl.BlockSpec(memory_space=pl.ANY)
    ws5 = [w.reshape(layers, side, side, *mat) for w, mat in zip(ws, mats)]
    mvs = [t.reshape(layers, *mat) for t, mat in zip((*ms, *vs), mats * 2)]
    out_shape = [jax.ShapeDtypeStruct(w.shape, BF) for w in ws5] + [jax.ShapeDtypeStruct(t.shape, F32) for t in mvs]
    dma = pltpu.SemaphoreType.DMA
    scratch = [
        pltpu.VMEM((3, 4, side, side, *gu), BF),
        pltpu.VMEM((2, 4, 3, side, *gu), BF),
        pltpu.VMEM((2, 4, 3, *gu), BF),
        pltpu.VMEM((4, 2, *gu), F32),
        pltpu.VMEM((4, *gu), BF),
        pltpu.VMEM((2, 4, *gu), BF),
        pltpu.VMEM((layers, side, side, per, 16, d), BF),
        pltpu.VMEM((2, 4, 3, side, *dn), BF),
        pltpu.VMEM((2, 4, 3, *dn), BF),
        pltpu.VMEM((2, 4, 2, *dn), F32),
        pltpu.VMEM((2, 4, *dn), BF),
        pltpu.VMEM((2, 4, *dn), BF),
        pltpu.VMEM((tokens, d), BF),
        pltpu.VMEM((d, tokens), BF),
        pltpu.VMEM((tokens, d), BF),
        pltpu.VMEM((tokens, d), F32),
        pltpu.VMEM((TILE, tokens), BF),
        pltpu.VMEM((tokens, 2 * TILE), BF),
        pltpu.VMEM((2, d, 2 * TILE), BF),
        pltpu.VMEM((2, TILE, d), BF),
        dma((2, 4, 12)), dma((2, 4, 12)), dma((2, 4, 12)), dma((2, 4, 12)),
        dma((4, 6)), dma((2, 4, 6)), dma((2, 3)), dma((6,)),
    ]
    res = pl.pallas_call(
        functools.partial(sync_kernel, side, tiles),
        out_shape=out_shape,
        in_specs=[hbm] * 18,
        out_specs=[hbm] * 9,
        scratch_shapes=scratch,
        compiler_params=pltpu.CompilerParams(collective_id=0, has_side_effects=True, vmem_limit_bytes=67043328),
        name="sync",
    )(*states, *ws, *ws5, *mvs)
    return [r.reshape(w.shape) for r, w in zip(res, (*ws, *ms, *vs))]


def solution(mesh):
    def step(x, dy, wg, wu, wd, *mv):
        x, dy = x[0], dy[0]
        a0, s0 = normed(x)
        g0, u0 = gate_up(a0, wg[0], wu[0])
        hid0 = (jax.nn.silu(g0) * u0).astype(BF)
        h1 = x + dot(hid0, wd[0], ((1,), (0,))).astype(BF)
        a1, s1 = normed(h1)
        states = (a1, a1.T, a0, a0.T, dy, h1)
        return tuple(synced(mesh, states, (wg, wu, wd), mv[:3], mv[3:]))

    rd, rep, shard = P(("rep", "dp")), P(), P(None, "dp", None)
    out, outs = P("rep"), P("rep", "dp", None)
    return jax.shard_map(
        step,
        mesh=mesh,
        in_specs=(rd, rd, rep, rep, rep, *[shard] * 6),
        out_specs=(out, out, out, *[outs] * 6),
        check_vma=False,
    )
```

```python
import functools
import math

import jax
import jax.numpy as jnp
from jax import lax
from jax.experimental import pallas as pl
from jax.experimental.pallas import tpu as pltpu
from jax.sharding import PartitionSpec as P

BF, F32 = jnp.bfloat16, jnp.float32
MESH = pl.DeviceIdType.MESH
TILE = 256


def dot(a, b, dims):
    return lax.dot_general(a, b, (dims, ((), ())), preferred_element_type=F32)


class Flow:
    pass


def sync_kernel(side, tiles, *refs):
    (a1, a1t, a0, a0t, dy_in, h1, h0t, wg2, wu2, wd2, wg, wu, wd, mg, mu, md, vg, vu, vd,
     og, ou, od, omg, omu, omd, ovg, ovu, ovd, kept,
     L, R1, R1c, R2, MV, W, NW, D, R1d, R2d, MVd, Wd, NWd, A, AT, DY, DA, HT, DGU, TW, TD,
     ss, rs, ssd, rsd, ls, lsd, lt, la, lk, lh) = refs
    tokens, d = A.shape
    block = 1024
    rep, me = lax.axis_index("rep"), lax.axis_index("dp")
    x, y = lax.div(me, side), lax.rem(me, side)
    xs, ys = ([lax.rem(v + n, side) for n in range(side)] for v in (x, y))

    def at(dx, dy):
        return (rep, xs[dx % side] * side + ys[dy % side])

    for src, dst, n in ((a1, A, 0), (dy_in, DY, 1), (a1t, AT, 2)):
        pltpu.make_async_copy(src, dst, la.at[n]).start()
    barrier = pltpu.get_barrier_semaphore()
    for dx, dy in ((1, 0), (-1, 0), (0, 1), (0, -1)):
        pl.semaphore_signal(barrier, inc=1, device_id=at(dx, dy), device_id_type=MESH)
    DA[...] = jnp.zeros_like(DA)
    pl.semaphore_wait(barrier, 4)

    def tile_of(c, t):
        g = 2 * t + c // 2
        past = g >= tiles
        return jnp.where(past, 0, 1), pl.multiple_of((g - jnp.where(past, tiles, 0)) * TILE, TILE)

    gu = Flow()
    gu.local = lambda c, t: L.at[lax.rem(t, 3), c]
    gu.r1 = lambda c, t, s: R1c.at[lax.rem(t, 3), c] if s == 2 else R1.at[lax.rem(t, 2), c, s]
    gu.r2 = lambda c, t, s: R2.at[lax.rem(t, 2), c, s]
    gu.nw = lambda c, t: NW.at[lax.rem(t, 2), c]
    gu.sems = lambda c, t, k: (ss.at[lax.rem(t, 2), c, k], rs.at[lax.rem(t, 2), c, k])
    gu.mv = lambda c, t: (MV.at[c, 0], MV.at[c, 1])
    gu.w = lambda c, t: W.at[c]
    gu.ls = lambda c, t, k: ls.at[c, k]

    def gu_out(c, t):
        layer, j = tile_of(c, t)
        return (og, ou)[c % 2].at[layer, :, :, :, pl.ds(j, TILE)]

    def gu_hbm(c, t):
        layer, j = tile_of(c, t)
        kind = c % 2
        cut = (layer, slice(None), pl.ds(j, TILE))
        return ((mg, mu)[kind].at[cut], (vg, vu)[kind].at[cut], (wg, wu)[kind].at[layer, x, y, :, pl.ds(j, TILE)],
                (omg, omu)[kind].at[cut], (ovg, ovu)[kind].at[cut])

    gu.out, gu.hbm = gu_out, gu_hbm

    def down(ab):
        fl = Flow()
        lane = lambda c: pl.ds(128 * (4 * ab + c), 128)
        fl.local = lambda c, t: D.at[t, :, :, :, :, lane(c)]
        fl.r1 = lambda c, t, s: R1d.at[ab, c, s]
        fl.r2 = lambda c, t, s: R2d.at[ab, c, s]
        fl.nw = lambda c, t: NWd.at[ab, c]
        fl.sems = lambda c, t, k: (ssd.at[ab, c, k], rsd.at[ab, c, k])
        fl.mv = lambda c, t: (MVd.at[ab, c, 0], MVd.at[ab, c, 1])
        fl.w = lambda c, t: Wd.at[ab, c]
        fl.ls = lambda c, t, k: lsd.at[ab, c, k]
        fl.out = lambda c, t: od.at[t, :, :, :, :, lane(c)]

        def hbm(c, t):
            cut = (t, slice(None), slice(None), lane(c))
            return md.at[cut], vd.at[cut], wd.at[t, x, y, :, :, lane(c)], omd.at[cut], ovd.at[cut]

        fl.hbm = hbm
        return fl

    downs = (down(0), down(1))

    toward = {(axis, sg): at(*((sg, 0) if axis == 0 else (0, sg))) for axis in (0, 1) for sg in (1, -1)}

    def stage(fl, c, t, k):
        first, sg = c < 2, (1, -1)[c % 2]
        r1, r2 = (xs, ys) if first else (ys, xs)
        p1, p2 = r1[0], r2[0]
        nb1, nb2 = (toward[0, sg], toward[1, sg]) if first else (toward[1, sg], toward[0, sg])
        loc = fl.local(c, t)

        def turned(r, n):
            return r[(-sg * n) % side]

        def chunk(ref, q):
            return ref.at[q] if first else ref.at[:, q]

        def sub(ref, q, q2):
            return ref.at[q, q2] if first else ref.at[q2, q]

        def copy(k):
            send, recv = fl.sems(c, t, k)
            if k < 3:
                src, dst, to = chunk(loc, turned(r1, 1 + k)), fl.r1(c, t, k), nb1
            elif k < 6:
                src, dst, to = sub(loc, p1, turned(r2, k - 2)), fl.r2(c, t, k - 3), nb2
            elif k < 9:
                dst, to = sub(fl.out(c, t), p1, turned(r2, k - 6)), nb2
                src = fl.nw(c, t) if k == 6 else dst
            else:
                dst, to = chunk(fl.out(c, t), turned(r1, k - 9)), nb1
                src = dst
            return pltpu.make_async_remote_copy(src, dst, send, recv, device_id=to, device_id_type=MESH)

        def locals_(ins_too):
            hm, hv, hw, hom, hov = fl.hbm(c, t)
            bm, bv = fl.mv(c, t)
            own = sub(fl.out(c, t), p1, p2)
            s = lambda n: fl.ls(c, t, n)
            if ins_too:
                return [pltpu.make_async_copy(a, b, s(n)) for n, (a, b) in enumerate(((hm, bm), (hv, bv), (hw, fl.w(c, t))))]
            return [pltpu.make_async_copy(a, b, s(3 + n)) for n, (a, b) in enumerate(((bm, hom), (bv, hov), (fl.nw(c, t), own)))]

        if k > 0:
            copy(k - 1).wait()
        if k in (1, 2):
            mine = chunk(loc, turned(r1, 1 + k))
            mine[...] = (mine[...].astype(F32) + fl.r1(c, t, k - 1)[...].astype(F32)).astype(BF)
        elif k in (3, 4, 5):
            q2 = turned(r2, k - 2)
            mine = sub(loc, p1, q2)
            total = mine[...].astype(F32) + fl.r1(c, t, 2).at[q2][...].astype(F32)
            if k > 3:
                total += fl.r2(c, t, k - 4)[...].astype(F32)
            mine[...] = total.astype(BF)
            if k == 4:
                for one in locals_(True):
                    one.start()
        elif k == 6:
            total = sub(loc, p1, p2)[...].astype(F32) + fl.r1(c, t, 2).at[p2][...].astype(F32)
            g = (total + fl.r2(c, t, 2)[...].astype(F32)).astype(BF).astype(F32)
            for one in locals_(True):
                one.wait()
            bm, bv = fl.mv(c, t)
            m = 0.9 * bm[...] + 0.1 * g
            v = 0.95 * bv[...] + 0.05 * g * g
            w = fl.w(c, t)[...].astype(F32)
            bm[...] = m
            bv[...] = v
            fl.nw(c, t)[...] = (w - 0.02 * (m * lax.rsqrt(v + 1e-8) + 0.1 * w)).astype(BF)
            for one in locals_(False):
                one.start()
        elif k == 7:
            for one in locals_(False):
                one.wait()
        if k < 12:
            copy(k).start()

    middle = 2 * ((2 * tiles + 2 + 5) // 6)
    last = 2 * tiles + middle

    def tile_loads(layer, j, par, down=True):
        cols = pl.ds(pl.multiple_of(j * TILE, TILE), TILE)
        loads = [pltpu.make_async_copy(wg2.at[layer, :, cols], TW.at[par, :, :TILE], lt.at[par, 0]),
                 pltpu.make_async_copy(wu2.at[layer, :, cols], TW.at[par, :, TILE:], lt.at[par, 1])]
        return loads + ([pltpu.make_async_copy(wd2.at[layer, cols, :], TD.at[par], lt.at[par, 2])] if down else [])

    def state_load(n):
        src, dst = ((a1, A), (dy_in, DY), (a1t, AT), (h1, A), (a0, A), (a0t, AT))[n]
        return pltpu.make_async_copy(src, dst, la.at[n])

    def keep(j, par):
        return pltpu.make_async_copy(DGU.at[par], kept.at[j], lk.at[par])

    def take(j, par):
        return pltpu.make_async_copy(kept.at[j], DGU.at[par], lk.at[par])

    def hidden_load(j):
        rows = pl.ds(pl.multiple_of(j * TILE, TILE), TILE)
        return pltpu.make_async_copy(h0t.at[rows, :], HT.at[lax.rem(j, 2)], lh.at[lax.rem(j, 2)])

    def forth_and_back(layer, j, par):
        def some(b, carry):
            rows = pl.ds(pl.multiple_of(b * block, block), block)
            both = dot(A[rows, :], TW[par], ((1,), (0,)))
            gate, up = both[:, :TILE], both[:, TILE:]
            d_hid = dot(DY[rows, :], TD[par], ((1,), (1,))).astype(BF).astype(F32)
            sig = jax.nn.sigmoid(gate)
            silu = gate * sig
            if layer == 1:
                HT[par, :, rows] = (silu * up).astype(BF).T
            DGU[par, rows, TILE:] = (d_hid * silu).astype(BF)
            DGU[par, rows, :TILE] = (d_hid * up * (sig * (1 + gate * (1 - sig)))).astype(BF)
            return carry

        lax.fori_loop(0, tokens // block, some, 0)

    def of_gate_and_up(g, par):
        slot, c = lax.div(g, 2), 2 * lax.rem(g, 2)
        both = dot(AT[...], DGU[par], ((1,), (0,))).astype(BF)
        L[lax.rem(slot, 3), c] = both[:, :TILE].reshape(side, side, -1, TILE)
        L[lax.rem(slot, 3), c + 1] = both[:, TILE:].reshape(side, side, -1, TILE)

    def of_down(layer, j, par):
        one = dot(HT[par], DY[...], ((1,), (0,))).astype(BF)
        per = D.shape[3]
        for i in range(TILE // 16):
            r = j * (TILE // 16) + i
            D[layer, lax.div(r, side * per), lax.rem(lax.div(r, per), side), lax.rem(r, per)] = one[16 * i : 16 * i + 16]

    def of_input(par):
        def some(b, carry):
            rows = pl.ds(pl.multiple_of(b * block, block), block)
            DA[rows, :] += dot(DGU[par, rows, :], TW[par], ((1,), (1,)))
            return carry

        lax.fori_loop(0, tokens // block, some, 0)

    def norm_back():
        def some(b, carry):
            rows = pl.ds(pl.multiple_of(b * 256, 256), 256)
            h = A[rows, :].astype(F32)
            scale = lax.rsqrt(jnp.mean(h * h, -1, keepdims=True) + 1e-6)
            da = DA[rows, :].astype(BF).astype(F32)
            inner = jnp.mean(h * da, -1, keepdims=True)
            back = (scale * (da - h * (scale * scale * inner))).astype(BF)
            DY[rows, :] = (DY[rows, :].astype(F32) + back.astype(F32)).astype(BF)
            return carry

        lax.fori_loop(0, tokens // 256, some, 0)

    def compute(q):
        turn, part = lax.div(q, 3), lax.rem(q, 3)
        first, second = turn < tiles, (turn >= tiles + middle) & (turn < last)
        g = jnp.where(first, turn, turn - middle)
        j, par = g - jnp.where(first, 0, tiles), lax.rem(g, 2)

        @pl.when((part == 0) & first)
        def _():
            @pl.when(g + 1 < tiles)
            def _():
                for one in tile_loads(1, j + 1, 1 - par):
                    one.start()

            for one in tile_loads(1, j, par):
                one.wait()

            @pl.when(g >= 2)
            def _():
                keep(j - 2, par).wait()

            forth_and_back(1, j, par)

            @pl.when(j < tiles - 1)
            def _():
                keep(j, par).start()

        @pl.when((part == 0) & second)
        def _():
            @pl.when(g + 1 < 2 * tiles)
            def _():
                for one in tile_loads(0, j + 1, 1 - par):
                    one.start()

            for one in tile_loads(0, j, par):
                one.wait()
            forth_and_back(0, j, par)

        @pl.when((part == 1) & (first | second))
        def _():
            of_gate_and_up(g, par)

        p = q - 3 * tiles
        h = p - tiles - 1

        @pl.when(((part == 2) & first) | ((h >= 0) & (h < tiles)))
        def _():
            @pl.when(~first)
            def _():
                @pl.when(h + 1 < tiles)
                def _():
                    hidden_load(h + 1).start()

                hidden_load(h).wait()

            of_down(jnp.where(first, 1, 0), jnp.where(first, j, h), jnp.where(first, par, lax.rem(h, 2)))

        @pl.when((p >= 0) & (p < tiles))
        def _():
            @pl.when(p == 0)
            def _():
                keep(tiles - 2, 1).wait()
                state_load(3).start()
                state_load(5).start()

            @pl.when(p > 0)
            def _():
                take(p - 1, lax.rem(p, 2)).wait()
                for one in tile_loads(1, p - 1, lax.rem(p, 2), False):
                    one.wait()

            @pl.when(p + 1 < tiles)
            def _():
                take(p, 1 - lax.rem(p, 2)).start()
                for one in tile_loads(1, p, 1 - lax.rem(p, 2), False):
                    one.start()

            of_input(lax.rem(p, 2))

        @pl.when(p == tiles)
        def _():
            hidden_load(0).start()
            for one in tile_loads(0, 0, tiles % 2):
                one.start()
            state_load(3).wait()
            norm_back()
            state_load(4).start()

        @pl.when(q == 3 * (tiles + middle) - 1)
        def _():
            state_load(4).wait()
            state_load(5).wait()

    def subround(q):
        six = lax.div(q, 6)
        place = q - 6 * six
        for z in range(6):

            @pl.when(place == z)
            def _():
                for k in range(12, -1, -1):
                    if (z - 2 - 2 * k) % 3 == 0:
                        turn = 2 * six + (z - 2 - 2 * k) // 3
                        second = turn >= tiles + middle
                        g = turn - jnp.where(second, middle, 0)

                        @pl.when(((turn >= 0) & (turn < tiles)) | (second & (turn < last)))
                        def _():
                            for c in (2 * (z % 2), 2 * (z % 2) + 1):
                                stage(gu, c, lax.div(g, 2), k)

        for ab in (0, 1):

            @pl.when((q >= 3 * tiles) & (lax.rem(q, 2) == (tiles + ab) % 2))
            def _():
                for k in range(12, -1, -1):
                    at1, at0 = 3 * tiles + ab + 2 * k, 3 * (tiles + middle) + ab + 2 * k

                    @pl.when((q == at1) | (q == at0))
                    def _():
                        for c in range(4):
                            stage(downs[ab], c, jnp.where(q == at1, 1, 0), k)

    def body(q, carry):
        compute(q)
        subround(q)
        return carry

    for one in tile_loads(1, 0, 0):
        one.start()
    for n in range(3):
        state_load(n).wait()
    lax.fori_loop(0, 3 * last + 2 + 2 * 12, body, 0)


def first_kernel(tiles, x_in, wg2, wu2, wd2, h1, a1, a1t, a0, a0t, h0t, X, A, AT, ACC, HN, HT, TW, TD, lt, lx, lh, lo):
    tokens, d = X.shape
    block, part = 1024, 512

    def tile_loads(j):
        par = lax.rem(j, 2)
        cols = pl.ds(pl.multiple_of(j * TILE, TILE), TILE)
        return (pltpu.make_async_copy(wg2.at[0, :, cols], TW.at[par, :, :TILE], lt.at[par, 0]),
                pltpu.make_async_copy(wu2.at[0, :, cols], TW.at[par, :, TILE:], lt.at[par, 1]),
                pltpu.make_async_copy(wd2.at[0, cols, :], TD.at[lax.rem(j, 3)], lt.at[par, 2]))

    def x_load(n):
        rows = pl.ds(pl.multiple_of(n * part, part), part)
        return pltpu.make_async_copy(x_in.at[rows, :], X.at[rows, :], lx.at[n])

    def hidden_out(j):
        return pltpu.make_async_copy(HT.at[j % 2], h0t.at[pl.ds(pl.multiple_of(j * TILE, TILE), TILE), :], lh.at[j % 2])

    def norm(rows, h):
        a = (h * lax.rsqrt(jnp.mean(h * h, -1, keepdims=True) + 1e-6)).astype(BF)
        A[rows, :] = a
        AT[:, rows] = a.T

    for n in range(tokens // part):
        x_load(n).start()
    for one in tile_loads(0):
        one.start()
    ACC[...] = jnp.zeros_like(ACC)
    HN[1] = jnp.zeros((tokens, TILE), BF)
    TD[2] = jnp.zeros((TILE, d), BF)

    def begin(n, carry):
        x_load(n).wait()
        rows = pl.ds(pl.multiple_of(n * part, part), part)
        norm(rows, X[rows, :].astype(F32))
        return carry

    lax.fori_loop(0, tokens // part, begin, 0)
    outs = [pltpu.make_async_copy(A, a0, lo.at[0]), pltpu.make_async_copy(AT, a0t, lo.at[1])]
    for one in outs:
        one.start()

    def turn(j, carry):
        par = j % 2

        @pl.when(j + 1 < tiles)
        def _():
            for one in tile_loads(j + 1):
                one.start()

        for one in tile_loads(j):
            one.wait()

        @pl.when(j >= 2)
        def _():
            hidden_out(j - 2).wait()

        def some(b, carry):
            rows = pl.ds(pl.multiple_of(b * block, block), block)
            both = dot(A[rows, :], TW[par], ((1,), (0,)))
            ACC[rows, :] += dot(HN[1 - par, rows, :], TD[lax.rem(j + 2, 3)], ((1,), (0,)))
            gate, up = both[:, :TILE], both[:, TILE:]
            hid = (gate * jax.nn.sigmoid(gate) * up).astype(BF)
            HN[par, rows, :] = hid
            HT[par, :, rows] = hid.T
            return carry

        lax.fori_loop(0, tokens // block, some, 0)
        hidden_out(j).start()
        return carry

    lax.fori_loop(0, tiles, turn, 0)

    def last_down(b, carry):
        rows = pl.ds(pl.multiple_of(b * block, block), block)
        ACC[rows, :] += dot(HN[(tiles - 1) % 2, rows, :], TD[(tiles - 1) % 3], ((1,), (0,)))
        return carry

    lax.fori_loop(0, tokens // block, last_down, 0)
    for one in outs:
        one.wait()
    hidden_out(tiles - 2).wait()
    hidden_out(tiles - 1).wait()

    def end(n, carry):
        rows = pl.ds(pl.multiple_of(n * part, part), part)
        h = (X[rows, :].astype(F32) + ACC[rows, :].astype(BF).astype(F32)).astype(BF)
        X[rows, :] = h
        norm(rows, h.astype(F32))
        return carry

    lax.fori_loop(0, tokens // part, end, 0)
    outs = [pltpu.make_async_copy(A, a1, lo.at[0]), pltpu.make_async_copy(AT, a1t, lo.at[1]), pltpu.make_async_copy(X, h1, lo.at[2])]
    for one in outs:
        one.start()
    for one in outs:
        one.wait()


def first(x, wg, wu, wd):
    tokens, d = x.shape
    ff = wg.shape[2]
    tiles = ff // TILE
    hbm = pl.BlockSpec(memory_space=pl.ANY)
    dma = pltpu.SemaphoreType.DMA
    wide, tall, hid = (jax.ShapeDtypeStruct(t, BF) for t in ((tokens, d), (d, tokens), (ff, tokens)))
    return pl.pallas_call(
        functools.partial(first_kernel, tiles),
        out_shape=[wide, wide, tall, wide, tall, hid],
        in_specs=[hbm] * 4,
        out_specs=[hbm] * 6,
        scratch_shapes=[
            pltpu.VMEM((tokens, d), BF), pltpu.VMEM((tokens, d), BF), pltpu.VMEM((d, tokens), BF), pltpu.VMEM((tokens, d), F32),
            pltpu.VMEM((2, tokens, TILE), BF), pltpu.VMEM((2, TILE, tokens), BF),
            pltpu.VMEM((2, d, 2 * TILE), BF), pltpu.VMEM((3, TILE, d), BF),
            dma((2, 3)), dma((4,)), dma((2,)), dma((3,)),
        ],
        compiler_params=pltpu.CompilerParams(vmem_limit_bytes=60 * 2**20),
        name="first",
    )(x, wg, wu, wd)


def synced(mesh, states, ws, ms, vs):
    n = mesh.shape["dp"]
    side = math.isqrt(n)
    layers, d, ff = ws[0].shape
    tokens = states[0].shape[0]
    tiles = ff // TILE
    rows, per = d // n, ff // n // 16
    gu, dn = (rows, TILE), (per, 16, 128)
    mats = ((rows, ff), (rows, ff), (per, 16, d))
    hbm = pl.BlockSpec(memory_space=pl.ANY)
    ws5 = [w.reshape(layers, side, side, *mat) for w, mat in zip(ws, mats)]
    mvs = [t.reshape(layers, *mat) for t, mat in zip((*ms, *vs), mats * 2)]
    out_shape = [jax.ShapeDtypeStruct(w.shape, BF) for w in ws5] + [jax.ShapeDtypeStruct(t.shape, F32) for t in mvs]
    out_shape.append(jax.ShapeDtypeStruct((tiles, tokens, 2 * TILE), BF))
    dma = pltpu.SemaphoreType.DMA
    scratch = [
        pltpu.VMEM((3, 4, side, side, *gu), BF),
        pltpu.VMEM((2, 4, 2, side, *gu), BF),
        pltpu.VMEM((3, 4, side, *gu), BF),
        pltpu.VMEM((2, 4, 3, *gu), BF),
        pltpu.VMEM((4, 2, *gu), F32),
        pltpu.VMEM((4, *gu), BF),
        pltpu.VMEM((2, 4, *gu), BF),
        pltpu.VMEM((layers, side, side, per, 16, d), BF),
        pltpu.VMEM((2, 4, 3, side, *dn), BF),
        pltpu.VMEM((2, 4, 3, *dn), BF),
        pltpu.VMEM((2, 4, 2, *dn), F32),
        pltpu.VMEM((2, 4, *dn), BF),
        pltpu.VMEM((2, 4, *dn), BF),
        pltpu.VMEM((tokens, d), BF),
        pltpu.VMEM((d, tokens), BF),
        pltpu.VMEM((tokens, d), BF),
        pltpu.VMEM((tokens, d), F32),
        pltpu.VMEM((2, TILE, tokens), BF),
        pltpu.VMEM((2, tokens, 2 * TILE), BF),
        pltpu.VMEM((2, d, 2 * TILE), BF),
        pltpu.VMEM((2, TILE, d), BF),
        dma((2, 4, 12)), dma((2, 4, 12)), dma((2, 4, 12)), dma((2, 4, 12)),
        dma((4, 6)), dma((2, 4, 6)), dma((2, 3)), dma((6,)), dma((2,)), dma((2,)),
    ]
    res = pl.pallas_call(
        functools.partial(sync_kernel, side, tiles),
        out_shape=out_shape,
        in_specs=[hbm] * 19,
        out_specs=[hbm] * 10,
        scratch_shapes=scratch,
        compiler_params=pltpu.CompilerParams(collective_id=0, has_side_effects=True, vmem_limit_bytes=67043328),
        name="sync",
    )(*states, *ws, *ws5, *mvs)
    return [r.reshape(w.shape) for r, w in zip(res[:9], (*ws, *ms, *vs))]


def solution(mesh):
    def step(x, dy, wg, wu, wd, *mv):
        x, dy = x[0], dy[0]
        h1, a1, a1t, a0, a0t, h0t = first(x, wg, wu, wd)
        states = (a1, a1t, a0, a0t, dy, h1, h0t)
        return tuple(synced(mesh, states, (wg, wu, wd), mv[:3], mv[3:]))

    rd, rep, shard = P(("rep", "dp")), P(), P(None, "dp", None)
    out, outs = P("rep"), P("rep", "dp", None)
    return jax.shard_map(
        step,
        mesh=mesh,
        in_specs=(rd, rd, rep, rep, rep, *[shard] * 6),
        out_specs=(out, out, out, *[outs] * 6),
        check_vma=False,
    )
```

```python
import functools
import math

import jax
import jax.numpy as jnp
from jax import lax
from jax.experimental import pallas as pl
from jax.experimental.pallas import tpu as pltpu
from jax.sharding import PartitionSpec as P

BF, F32 = jnp.bfloat16, jnp.float32
MESH = pl.DeviceIdType.MESH
TILE = 256


def dot(a, b, dims):
    return lax.dot_general(a, b, (dims, ((), ())), preferred_element_type=F32)


class Flow:
    pass


def sync_kernel(side, tiles, *refs):
    (x_in, dy_in, wg2, wu2, wd2, wg, wu, wd, mg, mu, md, vg, vu, vd,
     og, ou, od, omg, omu, omd, ovg, ovu, ovd, kept, a0, a0t, h0t,
     L, R1, R1c, R2, MV, W, NW, D, R1d, R2d, MVd, Wd, NWd, A, AT, DY, DA, HT, DGU, TW, TD,
     ss, rs, ssd, rsd, ls, lsd, lt, la, lk, lh, lx) = refs
    tokens, d = A.shape
    block = 1024
    rep, me = lax.axis_index("rep"), lax.axis_index("dp")
    x, y = lax.div(me, side), lax.rem(me, side)
    xs, ys = ([lax.rem(v + n, side) for n in range(side)] for v in (x, y))

    def at(dx, dy):
        return (rep, xs[dx % side] * side + ys[dy % side])

    barrier = pltpu.get_barrier_semaphore()
    for dx, dy in ((1, 0), (-1, 0), (0, 1), (0, -1)):
        pl.semaphore_signal(barrier, inc=1, device_id=at(dx, dy), device_id_type=MESH)
    def tile_of(c, t):
        g = 2 * t + c // 2
        past = g >= tiles
        return jnp.where(past, 0, 1), pl.multiple_of((g - jnp.where(past, tiles, 0)) * TILE, TILE)

    gu = Flow()
    gu.local = lambda c, t: L.at[lax.rem(t, 3), c]
    gu.r1 = lambda c, t, s: R1c.at[lax.rem(t, 3), c] if s == 2 else R1.at[lax.rem(t, 2), c, s]
    gu.r2 = lambda c, t, s: R2.at[lax.rem(t, 2), c, s]
    gu.nw = lambda c, t: NW.at[lax.rem(t, 2), c]
    gu.sems = lambda c, t, k: (ss.at[lax.rem(t, 2), c, k], rs.at[lax.rem(t, 2), c, k])
    gu.mv = lambda c, t: (MV.at[c, 0], MV.at[c, 1])
    gu.w = lambda c, t: W.at[c]
    gu.ls = lambda c, t, k: ls.at[c, k]

    def gu_out(c, t):
        layer, j = tile_of(c, t)
        return (og, ou)[c % 2].at[layer, :, :, :, pl.ds(j, TILE)]

    def gu_hbm(c, t):
        layer, j = tile_of(c, t)
        kind = c % 2
        cut = (layer, slice(None), pl.ds(j, TILE))
        return ((mg, mu)[kind].at[cut], (vg, vu)[kind].at[cut], (wg, wu)[kind].at[layer, x, y, :, pl.ds(j, TILE)],
                (omg, omu)[kind].at[cut], (ovg, ovu)[kind].at[cut])

    gu.out, gu.hbm = gu_out, gu_hbm

    def down(ab):
        fl = Flow()
        lane = lambda c: pl.ds(128 * (4 * ab + c), 128)
        fl.local = lambda c, t: D.at[t, :, :, :, :, lane(c)]
        fl.r1 = lambda c, t, s: R1d.at[ab, c, s]
        fl.r2 = lambda c, t, s: R2d.at[ab, c, s]
        fl.nw = lambda c, t: NWd.at[c]
        fl.sems = lambda c, t, k: (ssd.at[ab, c, k], rsd.at[ab, c, k])
        fl.mv = lambda c, t: (MVd.at[c, 0], MVd.at[c, 1])
        fl.w = lambda c, t: Wd.at[c]
        fl.ls = lambda c, t, k: lsd.at[ab, c, k]
        fl.out = lambda c, t: od.at[t, :, :, :, :, lane(c)]

        def hbm(c, t):
            cut = (t, slice(None), slice(None), lane(c))
            return md.at[cut], vd.at[cut], wd.at[t, x, y, :, :, lane(c)], omd.at[cut], ovd.at[cut]

        fl.hbm = hbm
        return fl

    downs = (down(0), down(1))

    toward = {(axis, sg): at(*((sg, 0) if axis == 0 else (0, sg))) for axis in (0, 1) for sg in (1, -1)}

    def stage(fl, c, t, k):
        first, sg = c < 2, (1, -1)[c % 2]
        r1, r2 = (xs, ys) if first else (ys, xs)
        p1, p2 = r1[0], r2[0]
        nb1, nb2 = (toward[0, sg], toward[1, sg]) if first else (toward[1, sg], toward[0, sg])
        loc = fl.local(c, t)

        def turned(r, n):
            return r[(-sg * n) % side]

        def chunk(ref, q):
            return ref.at[q] if first else ref.at[:, q]

        def sub(ref, q, q2):
            return ref.at[q, q2] if first else ref.at[q2, q]

        def copy(k):
            send, recv = fl.sems(c, t, k)
            if k < 3:
                src, dst, to = chunk(loc, turned(r1, 1 + k)), fl.r1(c, t, k), nb1
            elif k < 6:
                src, dst, to = sub(loc, p1, turned(r2, k - 2)), fl.r2(c, t, k - 3), nb2
            elif k < 9:
                dst, to = sub(fl.out(c, t), p1, turned(r2, k - 6)), nb2
                src = fl.nw(c, t) if k == 6 else dst
            else:
                dst, to = chunk(fl.out(c, t), turned(r1, k - 9)), nb1
                src = dst
            return pltpu.make_async_remote_copy(src, dst, send, recv, device_id=to, device_id_type=MESH)

        def locals_(ins_too):
            hm, hv, hw, hom, hov = fl.hbm(c, t)
            bm, bv = fl.mv(c, t)
            own = sub(fl.out(c, t), p1, p2)
            s = lambda n: fl.ls(c, t, n)
            if ins_too:
                return [pltpu.make_async_copy(a, b, s(n)) for n, (a, b) in enumerate(((hm, bm), (hv, bv), (hw, fl.w(c, t))))]
            return [pltpu.make_async_copy(a, b, s(3 + n)) for n, (a, b) in enumerate(((bm, hom), (bv, hov), (fl.nw(c, t), own)))]

        if k > 0:
            copy(k - 1).wait()
        if k in (1, 2):
            mine = chunk(loc, turned(r1, 1 + k))
            mine[...] = (mine[...].astype(F32) + fl.r1(c, t, k - 1)[...].astype(F32)).astype(BF)
        elif k in (3, 4, 5):
            q2 = turned(r2, k - 2)
            mine = sub(loc, p1, q2)
            total = mine[...].astype(F32) + fl.r1(c, t, 2).at[q2][...].astype(F32)
            if k > 3:
                total += fl.r2(c, t, k - 4)[...].astype(F32)
            mine[...] = total.astype(BF)
            if k == 4:
                for one in locals_(True):
                    one.start()
        elif k == 6:
            total = sub(loc, p1, p2)[...].astype(F32) + fl.r1(c, t, 2).at[p2][...].astype(F32)
            g = (total + fl.r2(c, t, 2)[...].astype(F32)).astype(BF).astype(F32)
            for one in locals_(True):
                one.wait()
            bm, bv = fl.mv(c, t)
            m = 0.9 * bm[...] + 0.1 * g
            v = 0.95 * bv[...] + 0.05 * g * g
            w = fl.w(c, t)[...].astype(F32)
            bm[...] = m
            bv[...] = v
            fl.nw(c, t)[...] = (w - 0.02 * (m * lax.rsqrt(v + 1e-8) + 0.1 * w)).astype(BF)
            for one in locals_(False):
                one.start()
        elif k == 7:
            for one in locals_(False):
                one.wait()
        if k < 12:
            copy(k).start()

    middle = 2 * ((2 * tiles + 2 + 5) // 6)
    last = 2 * tiles + middle

    def tile_loads(layer, j, par, down=True):
        cols = pl.ds(pl.multiple_of(j * TILE, TILE), TILE)
        loads = [pltpu.make_async_copy(wg2.at[layer, :, cols], TW.at[par, :, :TILE], lt.at[par, 0]),
                 pltpu.make_async_copy(wu2.at[layer, :, cols], TW.at[par, :, TILE:], lt.at[par, 1])]
        return loads + ([pltpu.make_async_copy(wd2.at[layer, cols, :], TD.at[par], lt.at[par, 2])] if down else [])

    def state_load(n):
        src, dst = ((dy_in, DY), (a0, A), (a0t, AT))[n]
        return pltpu.make_async_copy(src, dst, la.at[n])

    each = tokens // (side * side * 16)

    def forth():
        part = tokens // side

        def down_load(j):
            cols = pl.ds(pl.multiple_of(j * TILE, TILE), TILE)
            return [pltpu.make_async_copy(wd2.at[0, cols, :], TD.at[lax.rem(j, 3)], lt.at[lax.rem(j, 2), 2])]

        def loads(j):
            return tile_loads(0, j, lax.rem(j, 2), False) + down_load(j)

        def x_load(n):
            return pltpu.make_async_copy(x_in.at[n], D.at[0, n, :, pl.ds(0, each)], lx.at[n])

        def hidden_out(j):
            rows = pl.ds(pl.multiple_of(j * TILE, TILE), TILE)
            return pltpu.make_async_copy(HT.at[lax.rem(j, 2)], h0t.at[rows, :], lh.at[lax.rem(j, 2)])

        def norm(rows, h):
            a = (h * lax.rsqrt(jnp.mean(h * h, -1, keepdims=True) + 1e-6)).astype(BF)
            A[rows, :] = a
            AT[:, rows] = a.T

        for n in range(side):
            x_load(n).start()
        for one in loads(0):
            one.start()
        state_load(0).start()
        DA[...] = jnp.zeros_like(DA)
        DGU[1, :, :TILE] = jnp.zeros((tokens, TILE), BF)
        TD[2] = jnp.zeros((TILE, d), BF)

        def begin(n, carry):
            x_load(n).wait()
            norm(pl.ds(pl.multiple_of(n * part, part), part), D[0, n, :, :each].reshape(part, d).astype(F32))
            return carry

        lax.fori_loop(0, side, begin, 0)
        outs = [pltpu.make_async_copy(A, a0, la.at[1]), pltpu.make_async_copy(AT, a0t, la.at[2])]
        for one in outs:
            one.start()

        def turn(j, carry):
            par = lax.rem(j, 2)

            @pl.when(j + 1 < tiles)
            def _():
                for one in loads(j + 1):
                    one.start()

            for one in loads(j):
                one.wait()

            @pl.when(j >= 2)
            def _():
                hidden_out(j - 2).wait()

            def some(b, carry):
                rows = pl.ds(pl.multiple_of(b * block, block), block)
                both = dot(A[rows, :], TW[par], ((1,), (0,)))
                DA[rows, :] += dot(DGU[1 - par, rows, :TILE], TD[lax.rem(j + 2, 3)], ((1,), (0,)))
                gate, up = both[:, :TILE], both[:, TILE:]
                hid = (gate * jax.nn.sigmoid(gate) * up).astype(BF)
                DGU[par, rows, :TILE] = hid
                HT[par, :, rows] = hid.T
                return carry

            lax.fori_loop(0, tokens // block, some, 0)
            hidden_out(j).start()
            return carry

        lax.fori_loop(0, tiles, turn, 0)
        for one in tile_loads(1, 0, 0):
            one.start()

        def last_down(b, carry):
            rows = pl.ds(pl.multiple_of(b * block, block), block)
            DA[rows, :] += dot(DGU[(tiles - 1) % 2, rows, :TILE], TD[(tiles - 1) % 3], ((1,), (0,)))
            return carry

        lax.fori_loop(0, tokens // block, last_down, 0)
        for one in outs:
            one.wait()
        hidden_out(tiles - 2).wait()
        hidden_out(tiles - 1).wait()

        def end(n, carry):
            rows = pl.ds(pl.multiple_of(n * part, part), part)
            h = (D[0, n, :, :each].reshape(part, d).astype(F32) + DA[rows, :].astype(BF).astype(F32)).astype(BF)
            D[0, n, :, :each] = h.reshape(side, each, 16, d)
            DA[rows, :] = jnp.zeros((part, d), F32)
            norm(rows, h.astype(F32))
            return carry

        lax.fori_loop(0, side, end, 0)
        state_load(0).wait()

    def keep(j, par):
        return pltpu.make_async_copy(DGU.at[par], kept.at[j], lk.at[par])

    def take(j, par):
        return pltpu.make_async_copy(kept.at[j], DGU.at[par], lk.at[par])

    def hidden_load(j):
        rows = pl.ds(pl.multiple_of(j * TILE, TILE), TILE)
        return pltpu.make_async_copy(h0t.at[rows, :], HT.at[lax.rem(j, 2)], lh.at[lax.rem(j, 2)])

    def forth_and_back(layer, j, par):
        def some(b, carry):
            rows = pl.ds(pl.multiple_of(b * block, block), block)
            both = dot(A[rows, :], TW[par], ((1,), (0,)))
            gate, up = both[:, :TILE], both[:, TILE:]
            d_hid = dot(DY[rows, :], TD[par], ((1,), (1,))).astype(BF).astype(F32)
            sig = jax.nn.sigmoid(gate)
            silu = gate * sig
            if layer == 1:
                HT[par, :, rows] = (silu * up).astype(BF).T
            DGU[par, rows, TILE:] = (d_hid * silu).astype(BF)
            DGU[par, rows, :TILE] = (d_hid * up * (sig * (1 + gate * (1 - sig)))).astype(BF)
            return carry

        lax.fori_loop(0, tokens // block, some, 0)

    def of_gate_and_up(g, par):
        slot, c = lax.div(g, 2), 2 * lax.rem(g, 2)
        both = dot(AT[...], DGU[par], ((1,), (0,))).astype(BF)
        L[lax.rem(slot, 3), c] = both[:, :TILE].reshape(side, side, -1, TILE)
        L[lax.rem(slot, 3), c + 1] = both[:, TILE:].reshape(side, side, -1, TILE)

    def of_down(layer, j, par):
        one = dot(HT[par], DY[...], ((1,), (0,))).astype(BF)
        per = D.shape[3]
        for i in range(TILE // 16):
            r = j * (TILE // 16) + i
            D[layer, lax.div(r, side * per), lax.rem(lax.div(r, per), side), lax.rem(r, per)] = one[16 * i : 16 * i + 16]

    def of_input(par):
        def some(b, carry):
            rows = pl.ds(pl.multiple_of(b * block, block), block)
            DA[rows, :] += dot(DGU[par, rows, :], TW[par], ((1,), (1,)))
            return carry

        lax.fori_loop(0, tokens // block, some, 0)

    def norm_back():
        def some(n, carry):
            size = each * 16
            rows = pl.ds(pl.multiple_of(n * size, size), size)
            h = D[0, lax.div(n, side), lax.rem(n, side), :each].reshape(size, d).astype(F32)
            scale = lax.rsqrt(jnp.mean(h * h, -1, keepdims=True) + 1e-6)
            da = DA[rows, :].astype(BF).astype(F32)
            inner = jnp.mean(h * da, -1, keepdims=True)
            back = (scale * (da - h * (scale * scale * inner))).astype(BF)
            DY[rows, :] = (DY[rows, :].astype(F32) + back.astype(F32)).astype(BF)
            return carry

        lax.fori_loop(0, side * side, some, 0)

    def compute(q):
        turn, part = lax.div(q, 3), lax.rem(q, 3)
        first, second = turn < tiles, (turn >= tiles + middle) & (turn < last)
        g = jnp.where(first, turn, turn - middle)
        j, par = g - jnp.where(first, 0, tiles), lax.rem(g, 2)

        @pl.when((part == 0) & first)
        def _():
            @pl.when(g + 1 < tiles)
            def _():
                for one in tile_loads(1, j + 1, 1 - par):
                    one.start()

            for one in tile_loads(1, j, par):
                one.wait()

            @pl.when(g >= 2)
            def _():
                keep(j - 2, par).wait()

            forth_and_back(1, j, par)

            @pl.when(j < tiles - 1)
            def _():
                keep(j, par).start()

        @pl.when((part == 0) & second)
        def _():
            @pl.when(g + 1 < 2 * tiles)
            def _():
                for one in tile_loads(0, j + 1, 1 - par):
                    one.start()

            for one in tile_loads(0, j, par):
                one.wait()
            forth_and_back(0, j, par)

        @pl.when((part == 1) & (first | second))
        def _():
            of_gate_and_up(g, par)

        p = q - 3 * tiles
        h = p - tiles - 1

        @pl.when(((part == 2) & first) | ((h >= 0) & (h < tiles)))
        def _():
            @pl.when(~first)
            def _():
                @pl.when(h + 1 < tiles)
                def _():
                    hidden_load(h + 1).start()

                hidden_load(h).wait()

            of_down(jnp.where(first, 1, 0), jnp.where(first, j, h), jnp.where(first, par, lax.rem(h, 2)))

        @pl.when((p >= 0) & (p < tiles))
        def _():
            @pl.when(p == 0)
            def _():
                keep(tiles - 2, 1).wait()
                state_load(1).start()
                state_load(2).start()

            @pl.when(p > 0)
            def _():
                take(p - 1, lax.rem(p, 2)).wait()
                for one in tile_loads(1, p - 1, lax.rem(p, 2), False):
                    one.wait()

            @pl.when(p + 1 < tiles)
            def _():
                take(p, 1 - lax.rem(p, 2)).start()
                for one in tile_loads(1, p, 1 - lax.rem(p, 2), False):
                    one.start()

            of_input(lax.rem(p, 2))

        @pl.when(p == tiles)
        def _():
            hidden_load(0).start()
            for one in tile_loads(0, 0, tiles % 2):
                one.start()
            norm_back()

        @pl.when(q == 3 * (tiles + middle) - 1)
        def _():
            state_load(1).wait()
            state_load(2).wait()

    def subround(q):
        six = lax.div(q, 6)
        place = q - 6 * six
        for z in range(6):

            @pl.when(place == z)
            def _():
                for k in range(12, -1, -1):
                    if (z - 2 - 2 * k) % 3 == 0:
                        turn = 2 * six + (z - 2 - 2 * k) // 3
                        second = turn >= tiles + middle
                        g = turn - jnp.where(second, middle, 0)

                        @pl.when(((turn >= 0) & (turn < tiles)) | (second & (turn < last)))
                        def _():
                            for c in (2 * (z % 2), 2 * (z % 2) + 1):
                                stage(gu, c, lax.div(g, 2), k)

        for ab, at1, at0 in ((0, 3 * tiles + 4, 3 * (tiles + middle) + 10), (1, 3 * tiles + 11, 3 * (tiles + middle) + 29)):

            @pl.when((q >= at1) & (lax.rem(q, 2) == at1 % 2))
            def _():
                for k in range(12, -1, -1):
                    now1, now0 = q == at1 + 2 * k, q == at0 + 2 * k

                    @pl.when(now1 | now0)
                    def _():
                        for c in range(4):
                            stage(downs[ab], c, jnp.where(now1, 1, 0), k)

    def body(q, carry):
        compute(q)
        subround(q)
        return carry

    forth()
    pl.semaphore_wait(barrier, 4)
    lax.fori_loop(0, 3 * last + 2 + 2 * 12, body, 0)


def synced(mesh, states, ws, ms, vs):
    n = mesh.shape["dp"]
    side = math.isqrt(n)
    layers, d, ff = ws[0].shape
    x, dy = states
    tokens = x.shape[0]
    x = x.reshape(side, side, -1, 16, d)
    tiles = ff // TILE
    rows, per = d // n, ff // n // 16
    gu, dn = (rows, TILE), (per, 16, 128)
    mats = ((rows, ff), (rows, ff), (per, 16, d))
    hbm = pl.BlockSpec(memory_space=pl.ANY)
    ws5 = [w.reshape(layers, side, side, *mat) for w, mat in zip(ws, mats)]
    mvs = [t.reshape(layers, *mat) for t, mat in zip((*ms, *vs), mats * 2)]
    out_shape = [jax.ShapeDtypeStruct(w.shape, BF) for w in ws5] + [jax.ShapeDtypeStruct(t.shape, F32) for t in mvs]
    out_shape += [jax.ShapeDtypeStruct(t, BF) for t in ((tiles, tokens, 2 * TILE), (tokens, d), (d, tokens), (ff, tokens))]
    dma = pltpu.SemaphoreType.DMA
    scratch = [
        pltpu.VMEM((3, 4, side, side, *gu), BF),
        pltpu.VMEM((2, 4, 2, side, *gu), BF),
        pltpu.VMEM((3, 4, side, *gu), BF),
        pltpu.VMEM((2, 4, 3, *gu), BF),
        pltpu.VMEM((4, 2, *gu), F32),
        pltpu.VMEM((4, *gu), BF),
        pltpu.VMEM((2, 4, *gu), BF),
        pltpu.VMEM((layers, side, side, per, 16, d), BF),
        pltpu.VMEM((2, 4, 3, side, *dn), BF),
        pltpu.VMEM((2, 4, 3, *dn), BF),
        pltpu.VMEM((4, 2, *dn), F32),
        pltpu.VMEM((4, *dn), BF),
        pltpu.VMEM((4, *dn), BF),
        pltpu.VMEM((tokens, d), BF),
        pltpu.VMEM((d, tokens), BF),
        pltpu.VMEM((tokens, d), BF),
        pltpu.VMEM((tokens, d), F32),
        pltpu.VMEM((2, TILE, tokens), BF),
        pltpu.VMEM((2, tokens, 2 * TILE), BF),
        pltpu.VMEM((2, d, 2 * TILE), BF),
        pltpu.VMEM((3, TILE, d), BF),
        dma((2, 4, 12)), dma((2, 4, 12)), dma((2, 4, 12)), dma((2, 4, 12)),
        dma((4, 6)), dma((2, 4, 6)), dma((2, 3)), dma((3,)), dma((2,)), dma((2,)), dma((side,)),
    ]
    res = pl.pallas_call(
        functools.partial(sync_kernel, side, tiles),
        out_shape=out_shape,
        in_specs=[hbm] * 14,
        out_specs=[hbm] * 13,
        scratch_shapes=scratch,
        compiler_params=pltpu.CompilerParams(collective_id=0, has_side_effects=True, vmem_limit_bytes=67043328),
        name="sync",
    )(x, dy, *ws, *ws5, *mvs)
    return [r.reshape(w.shape) for r, w in zip(res[:9], (*ws, *ms, *vs))]


def solution(mesh):
    def step(x, dy, wg, wu, wd, *mv):
        x, dy = x[0], dy[0]
        states = (x, dy)
        return tuple(synced(mesh, states, (wg, wu, wd), mv[:3], mv[3:]))

    rd, rep, shard = P(("rep", "dp")), P(), P(None, "dp", None)
    out, outs = P("rep"), P("rep", "dp", None)
    return jax.shard_map(
        step,
        mesh=mesh,
        in_specs=(rd, rd, rep, rep, rep, *[shard] * 6),
        out_specs=(out, out, out, *[outs] * 6),
        check_vma=False,
    )
```
